256 devices in a mesh: groups: 4 (over y, x), ctx: 32 (over z), exp: 2 (over core).
Axes of the slice: x: 2, y: 2, z: 32, core: 2. Of those that a mesh axis runs over, the one named last changes fastest.
The devices are a block of a 4x8x32 slice.
Arguments:
- query_states: bfloat16 [8192, 3072], P(('groups', 'ctx'), 'exp'), parts along dimension 0, may hold values from -5 to 5
- key_states: bfloat16 [8192, 512], P(('groups', 'ctx'), 'exp'), parts along dimension 0, may hold values from -5 to 5
- value_states: bfloat16 [8192, 512], P(('groups', 'ctx'), 'exp'), parts along dimension 0, may hold values from -6 to 6
- residual: bfloat16 [8192, 3072], P(('groups', 'ctx'), 'exp'), parts along dimension 0, may hold values from -2 to 2
- norm_gain: float32 [3072], replicated, may hold values from 0.1 to 1.9
- expert_ids: int32 [8192, 2], P(('groups', 'ctx')), parts along dimension 0, may hold values from 0 to 7, all different within a row; in each aligned block of 32 rows (0 to 31, 32 to 63, ...) at most 12 rows name the same one
- route_weights: float32 [8192, 2], P(('groups', 'ctx')), parts along dimension 0, may hold values from 0.1 to 1
- w_gate: bfloat16 [3072, 65536], P(None, ('ctx', 'exp')), may hold values from -0.109375 to 0.109375
- w_down: bfloat16 [65536, 3072], P(('ctx', 'exp')), may hold values from -0.0625 to 0.0625
Outputs:
- mixed: bfloat16 [8192, 3072], P(('groups', 'ctx'), 'exp'), parts along dimension 0
The draws below stay inside these ranges and needn't reach their ends.
There are 4 independent parts, one for each index of `groups`. The reference program is written for one: setup_inputs(seed, part) draws one part's arguments, and reference() takes and returns one part's arrays. A program takes and returns all parts, laid end to end along the dimension named above; an argument that names none is the same for every part. Nothing has to cross between parts.
Inputs may be any that keep to these rules, and one draw needn't show every extreme that they name: `expert_ids`: each token names 2 different experts. In each aligned block of 32 tokens, at most 12 tokens name the same expert.
All inputs are finite; a program needn't handle non-finite values.
Results may differ from the reference program's by a relative error of at most 0.012.
Values may be sent and summed in bfloat16 or wider, within the bound.
No kernel may reach another device: no remote copies, remote signals or barrier semaphores. Data moves between devices by JAX's collectives and lax.ppermute only.
A program may use at most 64 MiB of HBM per device.

```python
import math
import jax
import jax.numpy as jnp
import numpy as np
from jax import lax

D = 3072
HEADS = 24
KV_HEADS = 4
HEAD_DIM = 128
EXPERTS = 8
TOP = 2
HALF_BLOCK = 32
HALF_CAP = 12
CAP = 24
TOKENS = 2048
FF = 8192
N_CTX = 32


def drawn_pair(key):
    base_key = jax.random.fold_in(key, 7)
    subkeys = jax.random.split(base_key, 2)
    query_shape = (TOKENS, HEADS * HEAD_DIM)
    key_shape = (TOKENS, KV_HEADS * HEAD_DIM)
    queries = jax.random.truncated_normal(subkeys[0], -5.0, 5.0, query_shape, jnp.float32)
    keys_drawn = jax.random.truncated_normal(subkeys[1], -5.0, 5.0, key_shape, jnp.float32)
    return (queries, keys_drawn)


def draw_query_states(key, part):
    return drawn_pair(key)[0].astype(jnp.bfloat16)


def draw_key_states(key, part):
    return drawn_pair(key)[1].astype(jnp.bfloat16)


def levels(key, extent, cuts, least, high):
    gain = 1.0
    for dim, parts in cuts:
        steps = jax.random.uniform(jax.random.fold_in(jax.random.fold_in(key, 6), dim), (parts,), jnp.float32, least / len(cuts), high / len(cuts))
        gain = gain * jnp.repeat(jnp.exp(steps), extent[dim] // parts).reshape((-1,) + (1,) * (len(extent) - 1 - dim))
    return gain


def shared_out(rng, own, number, rows, amount, top, limit, lean):
    order = jax.random.permutation(rng, amount)
    heavy_load, common = portions_of(amount, rows * top, limit, lean, True), portions_of(amount, rows * top, limit, lean, False)
    places = jnp.arange(amount)

    def named(lengths, offset_by):
        used = int((lengths > 0).sum())
        fixed = max(1, used // 4)
        shifted = fixed + (places - fixed + offset_by * (used - fixed)) % max(1, amount - fixed)
        return jnp.zeros((amount,), jnp.int32).at[order[jnp.where(places < fixed, places, shifted)]].set(jnp.asarray(lengths, jnp.int32))

    lengths = jnp.where(number % 4 == 0, named(heavy_load, number // 4), named(common, number - number // 4 - 1))
    mixed = jax.random.permutation(jax.random.fold_in(own, 3), amount)
    source_of, receiver = mixed[0:amount // 2 * 2:2], mixed[1:amount // 2 * 2:2]
    room = jnp.minimum(lengths[source_of] - 1, limit - lengths[receiver]) // 2
    room = jnp.where((source_of == order[0]) | (receiver == order[0]) | (lengths[receiver] == 0), 0, jnp.maximum(room, 0))
    shifted = jax.random.randint(jax.random.fold_in(own, 4), (amount // 2,), 0, 1 << 20) % (room + 1)
    lengths = lengths.at[source_of].add(-shifted).at[receiver].add(shifted)
    items = jnp.searchsorted(jnp.cumsum(lengths), jnp.arange(rows * top), side="right").astype(jnp.int32)
    table = items.reshape(top, rows).T
    table = table[jax.random.permutation(jax.random.fold_in(own, 1), rows)]
    offset_by = jax.random.randint(jax.random.fold_in(own, 2), (rows, 1), 0, top)
    return jnp.take_along_axis(table, (jnp.arange(top)[None, :] + offset_by) % top, axis=1)


def portions_of(number_of, total, most, lean, full):
    portions = [(1 << 20) // math.isqrt(standing ** lean) + 1 for standing in range(1, number_of + 1)]
    largest = most if full else min(most, max(-(-total // number_of), total * portions[0] // sum(portions)))
    least = 1 if total - largest >= number_of - 1 else 0
    counts, rest = [largest] + [least] * (number_of - 1), total - largest - least * (number_of - 1)
    while rest > 0:
        free = [i for i in range(1, number_of) if counts[i] < largest] or [i for i in range(1, number_of) if counts[i] < most]
        mass, left = sum([portions[i] for i in free]), rest
        for i in free:
            more = min(most - counts[i], max(1, left * portions[i] // mass), rest)
            counts[i] = counts[i] + more
            rest = rest - more
    return np.array(counts)


def gaussian(own_key, extent, spread, most, shards=(), kind=jnp.bfloat16):
    result = jax.random.normal(own_key, extent, jnp.float32) * spread
    if len(shards) > 0:
        result = levels(own_key, extent, shards, -0.22, 0.18) * result
    return jnp.clip(result, min=-most, max=most).astype(kind)


def setup_inputs(seed: int = 0, part: int = 0) -> dict:
    keys = jax.random.split(jax.random.key(seed), 10)
    part_splits = jax.random.split(jax.random.fold_in(keys[9], part), 10)
    query_states = draw_query_states(jax.random.fold_in(jax.random.fold_in(keys[9], part), 71), part)
    key_states = draw_key_states(jax.random.fold_in(jax.random.fold_in(keys[9], part), 71), part)
    value_states = gaussian(part_splits[2], (TOKENS, KV_HEADS * HEAD_DIM), 1.0, 6.0, ((0, 32), (1, 2)))
    residual = gaussian(part_splits[3], (TOKENS, D), 0.3, 2.0, ((0, 32), (1, 2)))
    norm_gain = jnp.clip(1.0 + 0.18 * jax.random.normal(keys[4], (D,), jnp.float32), 0.1, 1.9)
    expert_ids_keys = jax.random.split(jax.random.fold_in(part_splits[5], 1), TOKENS // HALF_BLOCK)
    expert_ids_turns = jax.random.permutation(jax.random.fold_in(part_splits[5], 3), TOKENS // HALF_BLOCK)
    expert_ids = jax.vmap(lambda own, number: shared_out(jax.random.fold_in(part_splits[5], 2), own, number, HALF_BLOCK, EXPERTS, TOP, HALF_CAP, 2))(expert_ids_keys, expert_ids_turns).reshape((TOKENS, TOP))
    route_weights = jnp.clip(0.1 + 0.9 * jax.random.uniform(part_splits[6], (TOKENS, TOP), jnp.float32) ** levels(part_splits[6], (TOKENS, TOP), ((0, 32),), -0.2, 0.2), 0.1, 1.0)
    w_gate = gaussian(keys[7], (D, EXPERTS * FF), D ** -0.5, 0.109375, ((1, 64),))
    w_down = gaussian(keys[8], (EXPERTS * FF, D), FF ** -0.5, 0.0625, ((0, 64),))
    return dict(query_states=query_states, key_states=key_states, value_states=value_states, residual=residual, norm_gain=norm_gain, expert_ids=expert_ids, route_weights=route_weights, w_gate=w_gate, w_down=w_down)


def reference(query_states, key_states, value_states, residual, norm_gain, expert_ids, route_weights, w_gate, w_down):
    per_group = HEADS // KV_HEADS
    tok_count = query_states.shape[0]
    query_heads = query_states.reshape(tok_count, KV_HEADS, per_group, HEAD_DIM).transpose(1, 0, 2, 3)
    key_heads = key_states.reshape(tok_count, KV_HEADS, HEAD_DIM).transpose(1, 0, 2)
    value_heads = value_states.reshape(tok_count, KV_HEADS, HEAD_DIM).transpose(1, 0, 2)
    position = jnp.arange(tok_count, dtype=jnp.int32)
    allowed = position[None, :] <= position[:, None]
    scaling = HEAD_DIM ** (-0.5)

    def one_head(operands):
        query_block, key_block, value_block = operands
        scores = jnp.einsum('qjd,kd->jqk', query_block.astype(jnp.float32), key_block.astype(jnp.float32)) * scaling
        row_max = lax.optimization_barrier(jnp.max(jnp.where(allowed[None], scores, -jnp.inf), axis=-1, keepdims=True))
        expo_terms = jnp.where(allowed[None], jnp.exp(scores - row_max), 0.0)
        totals = lax.optimization_barrier(jnp.sum(expo_terms, axis=-1))
        rounded = expo_terms.astype(jnp.bfloat16).astype(jnp.float32)
        weighted = jnp.einsum('jqk,kd->jqd', rounded, value_block.astype(jnp.float32))
        return (weighted / totals[..., None]).transpose(1, 0, 2)
    per_head = lax.map(one_head, (query_heads, key_heads, value_heads))
    attended = per_head.transpose(1, 0, 2, 3).reshape(tok_count, D)
    hidden = (residual.astype(jnp.float32) + attended).astype(jnp.bfloat16)
    hidden_float = hidden.astype(jnp.float32)
    mean_sq = lax.optimization_barrier(jnp.mean(jnp.square(hidden_float), axis=-1, keepdims=True))
    normed = (hidden_float * lax.rsqrt(mean_sq + 1e-05) * norm_gain.astype(jnp.float32)[None, :]).astype(jnp.bfloat16)
    mixed_sum = jnp.zeros((tok_count, D), jnp.float32)
    row_limit = N_CTX * CAP
    for expert in range(EXPERTS):
        hit_table = (expert_ids == expert).astype(jnp.int32)
        chosen = lax.optimization_barrier(jnp.sum(hit_table, axis=1))
        weight = lax.optimization_barrier(jnp.sum(route_weights * hit_table.astype(route_weights.dtype), axis=1))
        row_order = jnp.argsort(1 - chosen, stable=True)[:row_limit]
        rows = normed[row_order]
        gate_act = jax.nn.silu(jnp.dot(rows, w_gate[:, expert * FF:(expert + 1) * FF], preferred_element_type=jnp.float32)).astype(jnp.bfloat16)
        partial_value = jnp.dot(gate_act, w_down[expert * FF:(expert + 1) * FF], preferred_element_type=jnp.float32)
        mixed_sum = mixed_sum.at[row_order].add(partial_value * weight[row_order][:, None])
    return (hidden_float + mixed_sum).astype(jnp.bfloat16)
```

```python
import jax
import jax.numpy as jnp
from jax import lax
from jax.sharding import PartitionSpec as P

D = 3072
HEAD_DIM = 128
EXPERTS = 8
HALF_CAP = 12
KV_CHUNKS = 1
OUT_CHUNKS = 2
BACK_CHUNKS = 2
GROUPS = 4


def swap(x):
    return lax.ppermute(x, "exp", [(0, 1), (1, 0)])


def shift_pairs(n, cores=(0, 1)):
    pairs = []
    if 0 in cores:
        pairs += [(2 * i, 2 * ((i + 1) % n)) for i in range(n)]
    if 1 in cores:
        pairs += [(2 * i + 1, 2 * ((i - 1) % n) + 1) for i in range(n)]
    return pairs


def move(x, pairs):
    return lax.ppermute(x, ("ctx", "exp"), pairs)


def two_way(block, n):
    ahead = [(i, (i + 1) % n) for i in range(n)]
    back = [(i, (i - 1) % n) for i in range(n)]
    f, b = block, block
    from_behind, from_ahead = [], []
    for k in range(1, n // 2 + 1):
        f = lax.ppermute(f, "ctx", ahead)
        from_behind.append(f)
        if k < n // 2:
            b = lax.ppermute(b, "ctx", back)
            from_ahead.append(b)
    return from_behind, from_ahead


def routing_rows(expert_ids, route_weights, width):
    parts, rest = [], route_weights
    for _ in range(3):
        top = lax.reduce_precision(rest, 8, 7)
        parts.append(top)
        rest = rest - top
    rows = jnp.concatenate([expert_ids.astype(jnp.float32)] + parts, axis=1).T
    return jnp.pad(rows, ((0, 0), (0, width - rows.shape[1]))).astype(jnp.bfloat16)


def slots_of(routing, expert, capacity):
    ids = routing[:, 0:2].astype(jnp.float32)
    weights = routing.astype(jnp.float32)
    weights = weights[:, 2:4] + weights[:, 4:6] + weights[:, 6:8]
    named = ids == expert.astype(jnp.float32)
    token_weight = jnp.sum(jnp.where(named, weights, 0.0), axis=1)
    hit = jnp.any(named, axis=1)
    tokens = hit.shape[1]
    t = jnp.arange(tokens)
    half = t // (tokens // 2)
    before = ((t[:, None] < t[None, :]) & (half[:, None] == half[None, :])).astype(jnp.bfloat16)
    place = jnp.dot(hit.astype(jnp.bfloat16), before, preferred_element_type=jnp.float32)
    place = place.astype(jnp.int32) + (half * HALF_CAP)[None, :]
    place = jnp.where(hit, place, -1)
    marks = place[:, None, :] == jnp.arange(capacity, dtype=jnp.int32)[None, :, None]
    slot_weight = jnp.sum(jnp.where(marks, token_weight[:, None, :], 0.0), axis=2)
    return marks.astype(jnp.bfloat16), slot_weight


def body(
    query_states,
    key_states,
    value_states,
    residual,
    norm_gain,
    expert_ids,
    route_weights,
    w_gate,
    w_down,
):
    n_ctx = lax.axis_size("ctx")
    half_ring = n_ctx // 2
    ctx_rank = lax.axis_index("ctx")
    core = lax.axis_index("exp")
    tok_count = query_states.shape[0]
    kv_width = key_states.shape[1]
    kv_local = kv_width // HEAD_DIM
    q_local = query_states.shape[1] // HEAD_DIM
    per_group = q_local // kv_local
    capacity = 2 * HALF_CAP
    spread = n_ctx // EXPERTS
    expert = ctx_rank // spread

    own_block = jnp.concatenate(
        [
            jnp.concatenate([key_states, value_states], axis=1),
            routing_rows(expert_ids, route_weights, 2 * kv_width),
        ],
        axis=0,
    )
    from_behind, from_ahead = two_way(own_block, n_ctx)
    arrived = [own_block] + from_behind + from_ahead
    kv = jnp.concatenate([b[:tok_count] for b in arrived], axis=0)
    steps = jnp.concatenate(
        [-jnp.arange(half_ring + 1, dtype=jnp.int32), jnp.arange(1, half_ring, dtype=jnp.int32)]
    )
    shard_of = (ctx_rank + steps + n_ctx) % n_ctx
    key_pos = (shard_of[:, None] * tok_count + jnp.arange(tok_count, dtype=jnp.int32)).reshape(-1)

    query_heads = query_states.reshape(tok_count, kv_local, per_group, HEAD_DIM)
    query_pos = ctx_rank * tok_count + jnp.arange(tok_count, dtype=jnp.int32)
    key_heads = kv[:, :kv_width].reshape(-1, kv_local, HEAD_DIM)
    value_heads = kv[:, kv_width:].reshape(-1, kv_local, HEAD_DIM)
    scores = jnp.einsum(
        "qgjd,kgd->qgjk", query_heads, key_heads, preferred_element_type=jnp.float32
    ) * (HEAD_DIM ** (-0.5))
    allowed = (key_pos[None, :] <= query_pos[:, None])[:, None, None, :]
    row_max = jnp.max(jnp.where(allowed, scores, -jnp.inf), axis=-1)
    expo_terms = jnp.where(allowed, jnp.exp(scores - row_max[..., None]), 0.0)
    row_sum = jnp.sum(expo_terms, axis=-1)
    weighted = jnp.einsum(
        "qgjk,kgd->qgjd",
        expo_terms.astype(jnp.bfloat16),
        value_heads,
        preferred_element_type=jnp.float32,
    )
    attended = (weighted / row_sum[..., None]).reshape(tok_count, q_local * HEAD_DIM)
    hidden_half = (residual.astype(jnp.float32) + attended).astype(jnp.bfloat16)
    feat_half = hidden_half.shape[1]
    half_float = hidden_half.astype(jnp.float32)
    own_squares = jnp.sum(jnp.square(half_float), axis=1)
    squares = own_squares + swap(own_squares)
    inv_rms = lax.rsqrt(squares / D + 1e-05)
    gain_half = lax.dynamic_slice_in_dim(norm_gain, core * feat_half, feat_half)
    normed_half = (half_float * inv_rms[:, None] * gain_half[None, :]).astype(jnp.bfloat16)

    other_half = swap(normed_half)
    first = core == 0
    rows = jnp.concatenate(
        [jnp.where(first, normed_half, other_half), jnp.where(first, other_half, normed_half)],
        axis=1,
    )
    both = shift_pairs(n_ctx)
    per_chunk = tok_count // OUT_CHUNKS
    travelling = [rows[c * per_chunk : (c + 1) * per_chunk] for c in range(OUT_CHUNKS)]
    blocks = []
    for k in range(1, half_ring + 1):
        pairs = both if k < half_ring else shift_pairs(n_ctx, (0,))
        travelling = [move(x, pairs) for x in travelling]
        blocks.append(travelling)
    last = [
        jnp.where(first, x, rows[c * per_chunk : (c + 1) * per_chunk])
        for c, x in enumerate(blocks[-1])
    ]
    blocks[-1] = last

    own_routing = own_block[tok_count:, :tok_count]
    behind = jnp.stack([b[tok_count:, :tok_count] for b in from_behind])
    ahead = jnp.stack([b[tok_count:, :tok_count] for b in from_ahead] + [own_routing])
    mine_marks, _ = slots_of(jnp.where(first, behind, ahead), expert, capacity)
    peer_marks, peer_weight = slots_of(jnp.where(first, ahead, behind), expert, capacity)

    per = half_ring // GROUPS
    totals = []
    for g in range(GROUPS):
        lo = g * per
        arrived_rows = jnp.stack(
            [jnp.concatenate(blocks[k], axis=0) for k in range(lo, lo + per)]
        )
        packed = jnp.einsum(
            "bst,btd->bsd",
            mine_marks[lo : lo + per],
            arrived_rows,
            preferred_element_type=jnp.float32,
        ).astype(jnp.bfloat16)
        packed = packed.reshape(per * capacity, D)
        flat = jnp.concatenate([packed, swap(packed)], axis=0)
        act = jax.nn.silu(jnp.dot(flat, w_gate, preferred_element_type=jnp.float32))
        share = jnp.dot(act.astype(jnp.bfloat16), w_down, preferred_element_type=jnp.float32)
        from_peer = swap(share[: per * capacity].astype(jnp.bfloat16))
        total = share[per * capacity :] + from_peer.astype(jnp.float32)
        total = total * peer_weight[lo : lo + per].reshape(-1, 1)
        totals.append(total.astype(jnp.bfloat16).reshape(per, capacity, D))

    per_chunk = tok_count // BACK_CHUNKS

    def addend(k, c):
        marks = peer_marks[k - 1, :, c * per_chunk : (c + 1) * per_chunk]
        return jnp.einsum(
            "st,sd->td",
            marks,
            totals[(k - 1) // per][(k - 1) % per],
            preferred_element_type=jnp.float32,
        )

    running = [addend(half_ring, c).astype(jnp.bfloat16) for c in range(BACK_CHUNKS)]
    own_part = running
    for k in range(half_ring, 0, -1):
        pairs = both if k < half_ring else shift_pairs(n_ctx, (1,))
        running = [move(x, pairs) for x in running]
        if k > 1:
            running = [
                (x.astype(jnp.float32) + addend(k - 1, c)).astype(jnp.bfloat16)
                for c, x in enumerate(running)
            ]
    gathered = jnp.concatenate(running, axis=0).astype(jnp.float32)
    gathered = gathered + jnp.where(first, jnp.concatenate(own_part, axis=0), 0).astype(jnp.float32)
    low, high = gathered[:, :feat_half], gathered[:, feat_half:]
    kept = jnp.where(first, low, high)
    given = jnp.where(first, high, low).astype(jnp.bfloat16)
    branch = kept + swap(given).astype(jnp.float32)
    return (hidden_half.astype(jnp.float32) + branch).astype(jnp.bfloat16)


def solution(mesh):
    in_specs = (
        P(("groups", "ctx"), "exp"),
        P(("groups", "ctx"), "exp"),
        P(("groups", "ctx"), "exp"),
        P(("groups", "ctx"), "exp"),
        P(),
        P(("groups", "ctx"), None),
        P(("groups", "ctx"), None),
        P(None, ("ctx", "exp")),
        P(("ctx", "exp"), None),
    )
    out_specs = P(("groups", "ctx"), "exp")
    return jax.shard_map(body, mesh=mesh, in_specs=in_specs, out_specs=out_specs, check_vma=False)
```

```python
import functools

import jax
import jax.numpy as jnp
from jax import lax
from jax.experimental import pallas as pl
from jax.experimental.pallas import tpu as pltpu
from jax.sharding import PartitionSpec as P

D = 3072
HEAD_DIM = 128
EXPERTS = 8
HALF_CAP = 12
KEY_CHUNK = 512
OUT_CHUNKS = 2
BACK_CHUNKS = 2
GROUPS = 1
ADD_LANES = 768


def swap(x):
    return lax.ppermute(x, "exp", [(0, 1), (1, 0)])


def shift_pairs(n, cores=(0, 1)):
    pairs = []
    if 0 in cores:
        pairs += [(2 * i, 2 * ((i + 1) % n)) for i in range(n)]
    if 1 in cores:
        pairs += [(2 * i + 1, 2 * ((i - 1) % n) + 1) for i in range(n)]
    return pairs


def move(x, pairs):
    return lax.ppermute(x, ("ctx", "exp"), pairs)


def two_way(block, n):
    ahead = [(i, (i + 1) % n) for i in range(n)]
    back = [(i, (i - 1) % n) for i in range(n)]
    f, b = block, block
    from_behind, from_ahead = [], []
    for k in range(1, n // 2 + 1):
        f = lax.ppermute(f, "ctx", ahead)
        from_behind.append(f)
        if k < n // 2:
            b = lax.ppermute(b, "ctx", back)
            from_ahead.append(b)
    return from_behind, from_ahead


def routing_rows(expert_ids, route_weights, width):
    parts, rest = [], route_weights
    for _ in range(3):
        top = lax.reduce_precision(rest, 8, 7)
        parts.append(top)
        rest = rest - top
    rows = jnp.concatenate([expert_ids.astype(jnp.float32)] + parts, axis=1).T
    return jnp.pad(rows, ((0, 0), (0, width - rows.shape[1]))).astype(jnp.bfloat16)


def slots_of(routing, expert, capacity):
    ids = routing[:, 0:2].astype(jnp.float32)
    weights = routing.astype(jnp.float32)
    weights = weights[:, 2:4] + weights[:, 4:6] + weights[:, 6:8]
    named = ids == expert.astype(jnp.float32)
    token_weight = jnp.sum(jnp.where(named, weights, 0.0), axis=1)
    hit = jnp.any(named, axis=1)
    tokens = hit.shape[1]
    t = jnp.arange(tokens)
    half = t // (tokens // 2)
    before = ((t[:, None] < t[None, :]) & (half[:, None] == half[None, :])).astype(jnp.bfloat16)
    place = jnp.dot(hit.astype(jnp.bfloat16), before, preferred_element_type=jnp.float32)
    place = place.astype(jnp.int32) + (half * HALF_CAP)[None, :]
    place = jnp.where(hit, place, -1)
    marks = place[:, None, :] == jnp.arange(capacity, dtype=jnp.int32)[None, :, None]
    slot_weight = jnp.sum(jnp.where(marks, token_weight[:, None, :], 0.0), axis=2)
    return marks.astype(jnp.bfloat16), slot_weight


def attend_kernel(n_ctx, per_group, rank_ref, q_ref, res_ref, *refs):
    blocks = refs[:n_ctx]
    hidden_ref, squares_ref, routing_ref, k_ref, v_ref, s_ref = refs[n_ctx:]
    tok = q_ref.shape[0]
    kv_width = k_ref.shape[1]
    rows = per_group * tok
    n_keys = k_ref.shape[0]
    rank = rank_ref[0]
    for b in range(n_ctx):
        k_ref[b * tok : (b + 1) * tok, :] = blocks[b][:tok, :kv_width]
        v_ref[b * tok : (b + 1) * tok, :] = blocks[b][:tok, kv_width:]
        routing_ref[b] = blocks[b][tok:, : routing_ref.shape[2]]
    query_pos = rank * tok + lax.broadcasted_iota(jnp.int32, (rows, 1), 0) % tok
    squares = jnp.zeros((tok, HEAD_DIM), jnp.float32)
    for g in range(kv_width // HEAD_DIM):
        lanes = slice(g * HEAD_DIM, (g + 1) * HEAD_DIM)
        heads = [
            q_ref[:, (g * per_group + j) * HEAD_DIM : (g * per_group + j + 1) * HEAD_DIM]
            for j in range(per_group)
        ]
        q = jnp.concatenate(heads, axis=0)
        row_max = jnp.full((rows, 1), -1e30, jnp.float32)
        for c in range(n_keys // KEY_CHUNK):
            part = slice(c * KEY_CHUNK, (c + 1) * KEY_CHUNK)
            scores = lax.dot_general(
                q, k_ref[part, lanes], (((1,), (1,)), ((), ())), preferred_element_type=jnp.float32
            ) * (HEAD_DIM**-0.5)
            col = c * KEY_CHUNK + lax.broadcasted_iota(jnp.int32, (1, KEY_CHUNK), 1)
            block = col // tok
            step = jnp.where(block <= n_ctx // 2, -block, block - n_ctx // 2)
            shard = (rank + step + n_ctx) % n_ctx
            key_pos = shard * tok + col % tok
            scores = jnp.where(key_pos <= query_pos, scores, -1e30)
            s_ref[:, part] = scores
            row_max = jnp.maximum(row_max, jnp.max(scores, axis=1, keepdims=True))
        total = jnp.zeros((rows, 1), jnp.float32)
        acc = jnp.zeros((rows, HEAD_DIM), jnp.float32)
        for c in range(n_keys // KEY_CHUNK):
            part = slice(c * KEY_CHUNK, (c + 1) * KEY_CHUNK)
            p = jnp.exp(s_ref[:, part] - row_max)
            total = total + jnp.sum(p, axis=1, keepdims=True)
            acc = acc + jnp.dot(
                p.astype(jnp.bfloat16), v_ref[part, lanes], preferred_element_type=jnp.float32
            )
        attended = acc / total
        for j in range(per_group):
            out = slice((g * per_group + j) * HEAD_DIM, (g * per_group + j + 1) * HEAD_DIM)
            hidden = res_ref[:, out].astype(jnp.float32) + attended[j * tok : (j + 1) * tok]
            hidden = hidden.astype(jnp.bfloat16)
            hidden_ref[:, out] = hidden
            squares = squares + jnp.square(hidden.astype(jnp.float32))
    squares_ref[...] = jnp.broadcast_to(
        jnp.sum(squares, axis=1, keepdims=True), squares_ref.shape
    )


def attend(rank, queries, residual, blocks, kv_width):
    n_ctx = len(blocks)
    tok, width = queries.shape
    per_group = width // kv_width
    extra = blocks[0].shape[0] - tok
    vmem = pl.BlockSpec(memory_space=pltpu.VMEM)
    flops = 4 * tok * n_ctx * tok * width
    return pl.pallas_call(
        functools.partial(attend_kernel, n_ctx, per_group),
        out_shape=(
            jax.ShapeDtypeStruct((tok, width), jnp.bfloat16),
            jax.ShapeDtypeStruct((tok, HEAD_DIM), jnp.float32),
            jax.ShapeDtypeStruct((n_ctx, extra, HEAD_DIM), jnp.bfloat16),
        ),
        in_specs=[pl.BlockSpec(memory_space=pltpu.SMEM)] + [vmem] * (2 + n_ctx),
        out_specs=(vmem, vmem, vmem),
        scratch_shapes=[
            pltpu.VMEM((n_ctx * tok, kv_width), jnp.bfloat16),
            pltpu.VMEM((n_ctx * tok, kv_width), jnp.bfloat16),
            pltpu.VMEM((per_group * tok, n_ctx * tok), jnp.float32),
        ],
        cost_estimate=pl.CostEstimate(
            flops=flops, bytes_accessed=8 * tok * width, transcendentals=n_ctx * tok * tok * 12
        ),
        compiler_params=pltpu.CompilerParams(vmem_limit_bytes=24 * 1024 * 1024),
        name="attend",
    )(rank.reshape(1), queries, residual, *blocks)


def add_rows_kernel(block, row, x_ref, all_ref, out_ref):
    rows, width = x_ref.shape

    def tile(i, _):
        lanes = pl.ds(pl.multiple_of(i * ADD_LANES, ADD_LANES), ADD_LANES)
        more = all_ref[block, row : row + rows, lanes].astype(jnp.float32)
        out_ref[:, lanes] = (x_ref[:, lanes].astype(jnp.float32) + more).astype(jnp.bfloat16)
        return _

    lax.fori_loop(0, width // ADD_LANES, tile, 0)


def add_rows(x, addends, block, row):
    vmem = pl.BlockSpec(memory_space=pltpu.VMEM)
    return pl.pallas_call(
        functools.partial(add_rows_kernel, block, row),
        out_shape=jax.ShapeDtypeStruct(x.shape, x.dtype),
        in_specs=[vmem, vmem],
        out_specs=vmem,
        cost_estimate=pl.CostEstimate(flops=x.size, bytes_accessed=6 * x.size, transcendentals=0),
        compiler_params=pltpu.CompilerParams(vmem_limit_bytes=2 * 1024 * 1024),
        name="add_rows",
    )(x, addends)


def body(
    query_states,
    key_states,
    value_states,
    residual,
    norm_gain,
    expert_ids,
    route_weights,
    w_gate,
    w_down,
):
    n_ctx = lax.axis_size("ctx")
    half_ring = n_ctx // 2
    ctx_rank = lax.axis_index("ctx")
    core = lax.axis_index("exp")
    tok_count = query_states.shape[0]
    kv_width = key_states.shape[1]
    capacity = 2 * HALF_CAP
    spread = n_ctx // EXPERTS
    expert = ctx_rank // spread

    own_block = jnp.concatenate(
        [
            jnp.concatenate([key_states, value_states], axis=1),
            routing_rows(expert_ids, route_weights, 2 * kv_width),
        ],
        axis=0,
    )
    from_behind, from_ahead = two_way(own_block, n_ctx)
    arrived = [own_block] + from_behind + from_ahead
    hidden_half, own_squares, routing = attend(
        ctx_rank, query_states, residual, arrived, kv_width
    )
    feat_half = hidden_half.shape[1]

    first = core == 0
    other_half, other_squares = swap(hidden_half), swap(own_squares)
    squares = own_squares[:, :1] + other_squares[:, :1]
    inv_rms = lax.rsqrt(squares / D + 1e-05)
    whole = jnp.concatenate(
        [jnp.where(first, hidden_half, other_half), jnp.where(first, other_half, hidden_half)],
        axis=1,
    )
    rows = (whole.astype(jnp.float32) * inv_rms * norm_gain[None, :]).astype(jnp.bfloat16)
    both = shift_pairs(n_ctx)
    per_chunk = tok_count // OUT_CHUNKS
    travelling = [rows[c * per_chunk : (c + 1) * per_chunk] for c in range(OUT_CHUNKS)]
    blocks = []
    for k in range(1, half_ring + 1):
        pairs = both if k < half_ring else shift_pairs(n_ctx, (0,))
        travelling = [move(x, pairs) for x in travelling]
        blocks.append(travelling)
    last = [
        jnp.where(first, x, rows[c * per_chunk : (c + 1) * per_chunk])
        for c, x in enumerate(blocks[-1])
    ]
    blocks[-1] = last

    routing = routing[:, :, :tok_count]
    behind = routing[1 : half_ring + 1]
    ahead = jnp.concatenate([routing[half_ring + 1 :], routing[:1]], axis=0)
    mine_marks, _ = slots_of(jnp.where(first, behind, ahead), expert, capacity)
    peer_marks, peer_weight = slots_of(jnp.where(first, ahead, behind), expert, capacity)

    per = half_ring // GROUPS
    totals = []
    for g in range(GROUPS):
        lo = g * per
        arrived_rows = jnp.stack(
            [jnp.concatenate(blocks[k], axis=0) for k in range(lo, lo + per)]
        )
        packed = jnp.einsum(
            "bst,btd->bsd",
            mine_marks[lo : lo + per],
            arrived_rows,
            preferred_element_type=jnp.float32,
        ).astype(jnp.bfloat16)
        packed = packed.reshape(per * capacity, D)
        flat = jnp.concatenate([packed, swap(packed)], axis=0)
        act = jax.nn.silu(jnp.dot(flat, w_gate, preferred_element_type=jnp.float32))
        share = jnp.dot(act.astype(jnp.bfloat16), w_down, preferred_element_type=jnp.float32)
        from_peer = swap(share[: per * capacity].astype(jnp.bfloat16))
        total = share[per * capacity :] + from_peer.astype(jnp.float32)
        total = total * peer_weight[lo : lo + per].reshape(-1, 1)
        totals.append(total.astype(jnp.bfloat16).reshape(per, capacity, D))

    total = jnp.concatenate(totals, axis=0)
    per_chunk = tok_count // BACK_CHUNKS

    def in_token_form(lo, hi):
        return jnp.einsum(
            "kst,ksd->ktd", peer_marks[lo:hi], total[lo:hi], preferred_element_type=jnp.float32
        ).astype(jnp.bfloat16)

    farthest = in_token_form(half_ring - 1, half_ring)[0]
    addends = in_token_form(0, half_ring - 1)
    running = [farthest[c * per_chunk : (c + 1) * per_chunk] for c in range(BACK_CHUNKS)]
    for k in range(half_ring, 0, -1):
        pairs = both if k < half_ring else shift_pairs(n_ctx, (1,))
        running = [move(x, pairs) for x in running]
        if k > 1:
            running = [add_rows(x, addends, k - 2, c * per_chunk) for c, x in enumerate(running)]
    own_part = [farthest]
    gathered = jnp.concatenate(running, axis=0).astype(jnp.float32)
    gathered = gathered + jnp.where(first, jnp.concatenate(own_part, axis=0), 0).astype(jnp.float32)
    low, high = gathered[:, :feat_half], gathered[:, feat_half:]
    kept = jnp.where(first, low, high)
    given = jnp.where(first, high, low).astype(jnp.bfloat16)
    branch = kept + swap(given).astype(jnp.float32)
    return (hidden_half.astype(jnp.float32) + branch).astype(jnp.bfloat16)


def solution(mesh):
    in_specs = (
        P(("groups", "ctx"), "exp"),
        P(("groups", "ctx"), "exp"),
        P(("groups", "ctx"), "exp"),
        P(("groups", "ctx"), "exp"),
        P(),
        P(("groups", "ctx"), None),
        P(("groups", "ctx"), None),
        P(None, ("ctx", "exp")),
        P(("ctx", "exp"), None),
    )
    out_specs = P(("groups", "ctx"), "exp")
    return jax.shard_map(body, mesh=mesh, in_specs=in_specs, out_specs=out_specs, check_vma=False)
```

```python
import functools

import jax
import jax.numpy as jnp
from jax import lax
from jax.experimental import pallas as pl
from jax.experimental.pallas import tpu as pltpu
from jax.sharding import PartitionSpec as P

D = 3072
HEAD_DIM = 128
EXPERTS = 8
HALF_CAP = 12
KEY_CHUNK = 512
OUT_CHUNKS = 2
BACK_CHUNKS = 2
GROUPS = 1
ADD_LANES = 768


def swap(x):
    return lax.ppermute(x, "exp", [(0, 1), (1, 0)])


def shift_pairs(n, cores=(0, 1)):
    pairs = []
    if 0 in cores:
        pairs += [(2 * i, 2 * ((i + 1) % n)) for i in range(n)]
    if 1 in cores:
        pairs += [(2 * i + 1, 2 * ((i - 1) % n) + 1) for i in range(n)]
    return pairs


def move(x, pairs):
    return lax.ppermute(x, ("ctx", "exp"), pairs)


def two_way(block, n):
    ahead = [(i, (i + 1) % n) for i in range(n)]
    back = [(i, (i - 1) % n) for i in range(n)]
    f, b = block, block
    from_behind, from_ahead = [], []
    for k in range(1, n // 2 + 1):
        f = lax.ppermute(f, "ctx", ahead)
        from_behind.append(f)
        if k < n // 2:
            b = lax.ppermute(b, "ctx", back)
            from_ahead.append(b)
    return from_behind, from_ahead


def routing_rows(expert_ids, route_weights, width):
    parts, rest = [], route_weights
    for _ in range(3):
        top = lax.reduce_precision(rest, 8, 7)
        parts.append(top)
        rest = rest - top
    rows = jnp.concatenate([expert_ids.astype(jnp.float32)] + parts, axis=1).T
    return jnp.pad(rows, ((0, 0), (0, width - rows.shape[1]))).astype(jnp.bfloat16)


def slots_of(routing, expert, capacity):
    ids = routing[:, 0:2].astype(jnp.float32)
    weights = routing.astype(jnp.float32)
    weights = weights[:, 2:4] + weights[:, 4:6] + weights[:, 6:8]
    named = ids == expert.astype(jnp.float32)
    token_weight = jnp.sum(jnp.where(named, weights, 0.0), axis=1)
    hit = jnp.any(named, axis=1)
    tokens = hit.shape[1]
    t = jnp.arange(tokens)
    half = t // (tokens // 2)
    before = ((t[:, None] < t[None, :]) & (half[:, None] == half[None, :])).astype(jnp.bfloat16)
    place = jnp.dot(hit.astype(jnp.bfloat16), before, preferred_element_type=jnp.float32)
    place = place.astype(jnp.int32) + (half * HALF_CAP)[None, :]
    place = jnp.where(hit, place, -1)
    marks = place[:, None, :] == jnp.arange(capacity, dtype=jnp.int32)[None, :, None]
    slot_weight = jnp.sum(jnp.where(marks, token_weight[:, None, :], 0.0), axis=2)
    return marks.astype(jnp.bfloat16), slot_weight


def attend_kernel(n_ctx, per_group, rank_ref, q_ref, res_ref, *refs):
    blocks = refs[:n_ctx]
    hidden_ref, squares_ref, routing_ref, k_ref, v_ref, s_ref = refs[n_ctx:]
    tok = q_ref.shape[0]
    kv_width = k_ref.shape[1]
    rows = per_group * tok
    n_keys = k_ref.shape[0]
    rank = rank_ref[0]
    for b in range(n_ctx):
        k_ref[b * tok : (b + 1) * tok, :] = blocks[b][:tok, :kv_width]
        v_ref[b * tok : (b + 1) * tok, :] = blocks[b][:tok, kv_width:]
        routing_ref[b] = blocks[b][tok:, : routing_ref.shape[2]]
    query_pos = rank * tok + lax.broadcasted_iota(jnp.int32, (rows, 1), 0) % tok
    squares = jnp.zeros((tok, HEAD_DIM), jnp.float32)
    for g in range(kv_width // HEAD_DIM):
        lanes = slice(g * HEAD_DIM, (g + 1) * HEAD_DIM)
        heads = [
            q_ref[:, (g * per_group + j) * HEAD_DIM : (g * per_group + j + 1) * HEAD_DIM]
            for j in range(per_group)
        ]
        q = jnp.concatenate(heads, axis=0)
        row_max = jnp.full((rows, 1), -1e30, jnp.float32)
        for c in range(n_keys // KEY_CHUNK):
            part = slice(c * KEY_CHUNK, (c + 1) * KEY_CHUNK)
            scores = lax.dot_general(
                q, k_ref[part, lanes], (((1,), (1,)), ((), ())), preferred_element_type=jnp.float32
            ) * (HEAD_DIM**-0.5)
            col = c * KEY_CHUNK + lax.broadcasted_iota(jnp.int32, (1, KEY_CHUNK), 1)
            block = col // tok
            step = jnp.where(block <= n_ctx // 2, -block, block - n_ctx // 2)
            shard = (rank + step + n_ctx) % n_ctx
            key_pos = shard * tok + col % tok
            scores = jnp.where(key_pos <= query_pos, scores, -1e30)
            s_ref[:, part] = scores
            row_max = jnp.maximum(row_max, jnp.max(scores, axis=1, keepdims=True))
        total = jnp.zeros((rows, 1), jnp.float32)
        acc = jnp.zeros((rows, HEAD_DIM), jnp.float32)
        for c in range(n_keys // KEY_CHUNK):
            part = slice(c * KEY_CHUNK, (c + 1) * KEY_CHUNK)
            p = jnp.exp(s_ref[:, part] - row_max)
            total = total + jnp.sum(p, axis=1, keepdims=True)
            acc = acc + jnp.dot(
                p.astype(jnp.bfloat16), v_ref[part, lanes], preferred_element_type=jnp.float32
            )
        attended = acc / total
        for j in range(per_group):
            out = slice((g * per_group + j) * HEAD_DIM, (g * per_group + j + 1) * HEAD_DIM)
            hidden = res_ref[:, out].astype(jnp.float32) + attended[j * tok : (j + 1) * tok]
            hidden = hidden.astype(jnp.bfloat16)
            hidden_ref[:, out] = hidden
            squares = squares + jnp.square(hidden.astype(jnp.float32))
    squares_ref[...] = jnp.broadcast_to(
        jnp.sum(squares, axis=1, keepdims=True), squares_ref.shape
    )


def attend(rank, queries, residual, blocks, kv_width):
    n_ctx = len(blocks)
    tok, width = queries.shape
    per_group = width // kv_width
    extra = blocks[0].shape[0] - tok
    vmem = pl.BlockSpec(memory_space=pltpu.VMEM)
    flops = 4 * tok * n_ctx * tok * width
    return pl.pallas_call(
        functools.partial(attend_kernel, n_ctx, per_group),
        out_shape=(
            jax.ShapeDtypeStruct((tok, width), jnp.bfloat16),
            jax.ShapeDtypeStruct((tok, HEAD_DIM), jnp.float32),
            jax.ShapeDtypeStruct((n_ctx, extra, HEAD_DIM), jnp.bfloat16),
        ),
        in_specs=[pl.BlockSpec(memory_space=pltpu.SMEM)] + [vmem] * (2 + n_ctx),
        out_specs=(vmem, vmem, vmem),
        scratch_shapes=[
            pltpu.VMEM((n_ctx * tok, kv_width), jnp.bfloat16),
            pltpu.VMEM((n_ctx * tok, kv_width), jnp.bfloat16),
            pltpu.VMEM((per_group * tok, n_ctx * tok), jnp.float32),
        ],
        cost_estimate=pl.CostEstimate(
            flops=flops, bytes_accessed=8 * tok * width, transcendentals=n_ctx * tok * tok * 12
        ),
        compiler_params=pltpu.CompilerParams(vmem_limit_bytes=24 * 1024 * 1024),
        name="attend",
    )(rank.reshape(1), queries, residual, *blocks)


def add_rows_kernel(block, row, x_ref, all_ref, out_ref):
    rows, width = x_ref.shape

    def tile(i, _):
        lanes = pl.ds(pl.multiple_of(i * ADD_LANES, ADD_LANES), ADD_LANES)
        more = all_ref[block, row : row + rows, lanes].astype(jnp.float32)
        out_ref[:, lanes] = (x_ref[:, lanes].astype(jnp.float32) + more).astype(jnp.bfloat16)
        return _

    lax.fori_loop(0, width // ADD_LANES, tile, 0)


def add_rows(x, addends, block, row):
    vmem = pl.BlockSpec(memory_space=pltpu.VMEM)
    return pl.pallas_call(
        functools.partial(add_rows_kernel, block, row),
        out_shape=jax.ShapeDtypeStruct(x.shape, x.dtype),
        in_specs=[vmem, vmem],
        out_specs=vmem,
        cost_estimate=pl.CostEstimate(flops=x.size, bytes_accessed=6 * x.size, transcendentals=0),
        compiler_params=pltpu.CompilerParams(vmem_limit_bytes=2 * 1024 * 1024),
        name="add_rows",
    )(x, addends)


def expert_share(rows, w_gate, w_down):
    act = jax.nn.silu(jnp.dot(rows, w_gate, preferred_element_type=jnp.float32))
    return jnp.dot(act.astype(jnp.bfloat16), w_down, preferred_element_type=jnp.float32)


def body(
    query_states,
    key_states,
    value_states,
    residual,
    norm_gain,
    expert_ids,
    route_weights,
    w_gate,
    w_down,
):
    n_ctx = lax.axis_size("ctx")
    half_ring = n_ctx // 2
    ctx_rank = lax.axis_index("ctx")
    core = lax.axis_index("exp")
    tok_count = query_states.shape[0]
    kv_width = key_states.shape[1]
    capacity = 2 * HALF_CAP
    spread = n_ctx // EXPERTS
    expert = ctx_rank // spread

    own_block = jnp.concatenate(
        [
            jnp.concatenate([key_states, value_states], axis=1),
            routing_rows(expert_ids, route_weights, 2 * kv_width),
        ],
        axis=0,
    )
    from_behind, from_ahead = two_way(own_block, n_ctx)
    arrived = [own_block] + from_behind + from_ahead
    hidden_half, own_squares, routing = attend(
        ctx_rank, query_states, residual, arrived, kv_width
    )
    feat_half = hidden_half.shape[1]

    first = core == 0
    other_half, other_squares = swap(hidden_half), swap(own_squares)
    squares = own_squares[:, :1] + other_squares[:, :1]
    inv_rms = lax.rsqrt(squares / D + 1e-05)
    whole = jnp.concatenate(
        [jnp.where(first, hidden_half, other_half), jnp.where(first, other_half, hidden_half)],
        axis=1,
    )
    rows = (whole.astype(jnp.float32) * inv_rms * norm_gain[None, :]).astype(jnp.bfloat16)
    both = shift_pairs(n_ctx)
    per_chunk = tok_count // OUT_CHUNKS
    travelling = [rows[c * per_chunk : (c + 1) * per_chunk] for c in range(OUT_CHUNKS)]
    blocks = []
    for k in range(1, half_ring + 1):
        pairs = both if k < half_ring else shift_pairs(n_ctx, (0,))
        travelling = [move(x, pairs) for x in travelling]
        blocks.append(travelling)
        if k < half_ring:
            travelling = list(travelling)
            for c in range(1, OUT_CHUNKS):
                travelling[c], blocks[-1][c - 1] = lax.optimization_barrier(
                    (travelling[c], blocks[-1][c - 1])
                )
            if k > 1:
                travelling[0], blocks[-2][-1] = lax.optimization_barrier(
                    (travelling[0], blocks[-2][-1])
                )
    last = [
        jnp.where(first, x, rows[c * per_chunk : (c + 1) * per_chunk])
        for c, x in enumerate(blocks[-1])
    ]
    blocks[-1] = last

    routing = routing[:, :, :tok_count]
    behind = routing[1 : half_ring + 1]
    ahead = jnp.concatenate([routing[half_ring + 1 :], routing[:1]], axis=0)
    mine_marks, _ = slots_of(jnp.where(first, behind, ahead), expert, capacity)
    peer_marks, peer_weight = slots_of(jnp.where(first, ahead, behind), expert, capacity)

    per = half_ring // GROUPS
    totals = []
    for g in range(GROUPS):
        lo = g * per
        arrived_rows = jnp.stack(
            [jnp.concatenate(blocks[k], axis=0) for k in range(lo, lo + per)]
        )
        packed = jnp.einsum(
            "bst,btd->bsd",
            mine_marks[lo : lo + per],
            arrived_rows,
            preferred_element_type=jnp.float32,
        ).astype(jnp.bfloat16)
        packed = packed.reshape(per * capacity, D)
        from_peer = swap(packed)
        sent_back = swap(expert_share(packed, w_gate, w_down).astype(jnp.bfloat16))
        share = lax.optimization_barrier(expert_share(from_peer, w_gate, w_down))
        total = share + sent_back.astype(jnp.float32)
        total = total * peer_weight[lo : lo + per].reshape(-1, 1)
        totals.append(total.astype(jnp.bfloat16).reshape(per, capacity, D))

    total = jnp.concatenate(totals, axis=0)
    per_chunk = tok_count // BACK_CHUNKS

    def in_token_form(lo, hi):
        return jnp.einsum(
            "kst,ksd->ktd", peer_marks[lo:hi], total[lo:hi], preferred_element_type=jnp.float32
        ).astype(jnp.bfloat16)

    farthest = in_token_form(half_ring - 1, half_ring)[0]
    addends = in_token_form(0, half_ring - 1)
    running = [farthest[c * per_chunk : (c + 1) * per_chunk] for c in range(BACK_CHUNKS)]
    for k in range(half_ring, 0, -1):
        pairs = both if k < half_ring else shift_pairs(n_ctx, (1,))
        running = [move(x, pairs) for x in running]
        if k > 1:
            running = [add_rows(x, addends, k - 2, c * per_chunk) for c, x in enumerate(running)]
    own_part = [farthest]
    gathered = jnp.concatenate(running, axis=0).astype(jnp.float32)
    gathered = gathered + jnp.where(first, jnp.concatenate(own_part, axis=0), 0).astype(jnp.float32)
    low, high = gathered[:, :feat_half], gathered[:, feat_half:]
    kept = jnp.where(first, low, high)
    given = jnp.where(first, high, low).astype(jnp.bfloat16)
    branch = kept + swap(given).astype(jnp.float32)
    return (hidden_half.astype(jnp.float32) + branch).astype(jnp.bfloat16)


def solution(mesh):
    in_specs = (
        P(("groups", "ctx"), "exp"),
        P(("groups", "ctx"), "exp"),
        P(("groups", "ctx"), "exp"),
        P(("groups", "ctx"), "exp"),
        P(),
        P(("groups", "ctx"), None),
        P(("groups", "ctx"), None),
        P(None, ("ctx", "exp")),
        P(("ctx", "exp"), None),
    )
    out_specs = P(("groups", "ctx"), "exp")
    return jax.shard_map(body, mesh=mesh, in_specs=in_specs, out_specs=out_specs, check_vma=False)
```

```python
import functools

import jax
import jax.numpy as jnp
from jax import lax
from jax.experimental import pallas as pl
from jax.experimental.pallas import tpu as pltpu
from jax.sharding import PartitionSpec as P

D = 3072
HEAD_DIM = 128
EXPERTS = 8
HALF_CAP = 12
KEY_CHUNK = 512
OUT_CHUNKS = 2
BACK_CHUNKS = 3
GROUPS = 1
ADD_LANES = 512


def swap(x):
    return lax.ppermute(x, "exp", [(0, 1), (1, 0)])


def shift_pairs(n, cores=(0, 1)):
    pairs = []
    if 0 in cores:
        pairs += [(2 * i, 2 * ((i + 1) % n)) for i in range(n)]
    if 1 in cores:
        pairs += [(2 * i + 1, 2 * ((i - 1) % n) + 1) for i in range(n)]
    return pairs


def move(x, pairs):
    return lax.ppermute(x, ("ctx", "exp"), pairs)


def two_way(block, n):
    ahead = [(i, (i + 1) % n) for i in range(n)]
    back = [(i, (i - 1) % n) for i in range(n)]
    f, b = block, block
    from_behind, from_ahead = [], []
    for k in range(1, n // 2 + 1):
        f = lax.ppermute(f, "ctx", ahead)
        from_behind.append(f)
        if k < n // 2:
            b = lax.ppermute(b, "ctx", back)
            from_ahead.append(b)
    return from_behind, from_ahead


def routing_rows(expert_ids, route_weights, width):
    parts, rest = [], route_weights
    for _ in range(3):
        top = lax.reduce_precision(rest, 8, 7)
        parts.append(top)
        rest = rest - top
    rows = jnp.concatenate([expert_ids.astype(jnp.float32)] + parts, axis=1).T
    return jnp.pad(rows, ((0, 0), (0, width - rows.shape[1]))).astype(jnp.bfloat16)


def slots_of(routing, expert, capacity):
    ids = routing[:, 0:2].astype(jnp.float32)
    weights = routing.astype(jnp.float32)
    weights = weights[:, 2:4] + weights[:, 4:6] + weights[:, 6:8]
    named = ids == expert.astype(jnp.float32)
    token_weight = jnp.sum(jnp.where(named, weights, 0.0), axis=1)
    hit = jnp.any(named, axis=1)
    tokens = hit.shape[1]
    t = jnp.arange(tokens)
    half = t // (tokens // 2)
    before = ((t[:, None] < t[None, :]) & (half[:, None] == half[None, :])).astype(jnp.bfloat16)
    place = jnp.dot(hit.astype(jnp.bfloat16), before, preferred_element_type=jnp.float32)
    place = place.astype(jnp.int32) + (half * HALF_CAP)[None, :]
    place = jnp.where(hit, place, -1)
    marks = place[:, None, :] == jnp.arange(capacity, dtype=jnp.int32)[None, :, None]
    slot_weight = jnp.sum(jnp.where(marks, token_weight[:, None, :], 0.0), axis=2)
    return marks.astype(jnp.bfloat16), slot_weight


def attend_kernel(n_ctx, per_group, rank_ref, q_ref, res_ref, *refs):
    blocks = refs[:n_ctx]
    hidden_ref, squares_ref, routing_ref, k_ref, v_ref, s_ref = refs[n_ctx:]
    tok = q_ref.shape[0]
    kv_width = k_ref.shape[1]
    rows = per_group * tok
    n_keys = k_ref.shape[0]
    rank = rank_ref[0]
    for b in range(n_ctx):
        k_ref[b * tok : (b + 1) * tok, :] = blocks[b][:tok, :kv_width]
        v_ref[b * tok : (b + 1) * tok, :] = blocks[b][:tok, kv_width:]
        routing_ref[b] = blocks[b][tok:, : routing_ref.shape[2]]
    query_pos = rank * tok + lax.broadcasted_iota(jnp.int32, (rows, 1), 0) % tok
    squares = jnp.zeros((tok, HEAD_DIM), jnp.float32)
    for g in range(kv_width // HEAD_DIM):
        lanes = slice(g * HEAD_DIM, (g + 1) * HEAD_DIM)
        heads = [
            q_ref[:, (g * per_group + j) * HEAD_DIM : (g * per_group + j + 1) * HEAD_DIM]
            for j in range(per_group)
        ]
        q = jnp.concatenate(heads, axis=0)
        row_max = jnp.full((rows, 1), -1e30, jnp.float32)
        for c in range(n_keys // KEY_CHUNK):
            part = slice(c * KEY_CHUNK, (c + 1) * KEY_CHUNK)
            scores = lax.dot_general(
                q, k_ref[part, lanes], (((1,), (1,)), ((), ())), preferred_element_type=jnp.float32
            ) * (HEAD_DIM**-0.5)
            col = c * KEY_CHUNK + lax.broadcasted_iota(jnp.int32, (1, KEY_CHUNK), 1)
            block = col // tok
            step = jnp.where(block <= n_ctx // 2, -block, block - n_ctx // 2)
            shard = (rank + step + n_ctx) % n_ctx
            key_pos = shard * tok + col % tok
            scores = jnp.where(key_pos <= query_pos, scores, -1e30)
            s_ref[:, part] = scores
            row_max = jnp.maximum(row_max, jnp.max(scores, axis=1, keepdims=True))
        total = jnp.zeros((rows, 1), jnp.float32)
        acc = jnp.zeros((rows, HEAD_DIM), jnp.float32)
        for c in range(n_keys // KEY_CHUNK):
            part = slice(c * KEY_CHUNK, (c + 1) * KEY_CHUNK)
            p = jnp.exp(s_ref[:, part] - row_max)
            total = total + jnp.sum(p, axis=1, keepdims=True)
            acc = acc + jnp.dot(
                p.astype(jnp.bfloat16), v_ref[part, lanes], preferred_element_type=jnp.float32
            )
        attended = acc / total
        for j in range(per_group):
            out = slice((g * per_group + j) * HEAD_DIM, (g * per_group + j + 1) * HEAD_DIM)
            hidden = res_ref[:, out].astype(jnp.float32) + attended[j * tok : (j + 1) * tok]
            hidden = hidden.astype(jnp.bfloat16)
            hidden_ref[:, out] = hidden
            squares = squares + jnp.square(hidden.astype(jnp.float32))
    squares_ref[...] = jnp.broadcast_to(
        jnp.sum(squares, axis=1, keepdims=True), squares_ref.shape
    )


def attend(rank, queries, residual, blocks, kv_width):
    n_ctx = len(blocks)
    tok, width = queries.shape
    per_group = width // kv_width
    extra = blocks[0].shape[0] - tok
    vmem = pl.BlockSpec(memory_space=pltpu.VMEM)
    flops = 4 * tok * n_ctx * tok * width
    return pl.pallas_call(
        functools.partial(attend_kernel, n_ctx, per_group),
        out_shape=(
            jax.ShapeDtypeStruct((tok, width), jnp.bfloat16),
            jax.ShapeDtypeStruct((tok, HEAD_DIM), jnp.float32),
            jax.ShapeDtypeStruct((n_ctx, extra, HEAD_DIM), jnp.bfloat16),
        ),
        in_specs=[pl.BlockSpec(memory_space=pltpu.SMEM)] + [vmem] * (2 + n_ctx),
        out_specs=(vmem, vmem, vmem),
        scratch_shapes=[
            pltpu.VMEM((n_ctx * tok, kv_width), jnp.bfloat16),
            pltpu.VMEM((n_ctx * tok, kv_width), jnp.bfloat16),
            pltpu.VMEM((per_group * tok, n_ctx * tok), jnp.float32),
        ],
        cost_estimate=pl.CostEstimate(
            flops=flops, bytes_accessed=8 * tok * width, transcendentals=n_ctx * tok * tok * 12
        ),
        compiler_params=pltpu.CompilerParams(vmem_limit_bytes=24 * 1024 * 1024),
        name="attend",
    )(rank.reshape(1), queries, residual, *blocks)


def add_rows_kernel(block, first_lane, x_ref, all_ref, out_ref):
    width = x_ref.shape[1]

    def tile(i, _):
        lanes = pl.ds(pl.multiple_of(i * ADD_LANES, ADD_LANES), ADD_LANES)
        theirs = pl.ds(pl.multiple_of(first_lane + i * ADD_LANES, ADD_LANES), ADD_LANES)
        more = all_ref[block, :, theirs].astype(jnp.float32)
        out_ref[:, lanes] = (x_ref[:, lanes].astype(jnp.float32) + more).astype(jnp.bfloat16)
        return _

    lax.fori_loop(0, width // ADD_LANES, tile, 0)


def add_rows(x, addends, block, first_lane):
    vmem = pl.BlockSpec(memory_space=pltpu.VMEM)
    return pl.pallas_call(
        functools.partial(add_rows_kernel, block, first_lane),
        out_shape=jax.ShapeDtypeStruct(x.shape, x.dtype),
        in_specs=[vmem, vmem],
        out_specs=vmem,
        cost_estimate=pl.CostEstimate(flops=x.size, bytes_accessed=6 * x.size, transcendentals=0),
        compiler_params=pltpu.CompilerParams(vmem_limit_bytes=2 * 1024 * 1024),
        name="add_rows",
    )(x, addends)


def expert_share(rows, w_gate, w_down):
    act = jax.nn.silu(jnp.dot(rows, w_gate, preferred_element_type=jnp.float32))
    act = lax.optimization_barrier(act.astype(jnp.bfloat16))
    return jnp.dot(act, w_down, preferred_element_type=jnp.float32)


def body(
    query_states,
    key_states,
    value_states,
    residual,
    norm_gain,
    expert_ids,
    route_weights,
    w_gate,
    w_down,
):
    n_ctx = lax.axis_size("ctx")
    half_ring = n_ctx // 2
    ctx_rank = lax.axis_index("ctx")
    core = lax.axis_index("exp")
    tok_count = query_states.shape[0]
    kv_width = key_states.shape[1]
    capacity = 2 * HALF_CAP
    spread = n_ctx // EXPERTS
    expert = ctx_rank // spread

    own_block = jnp.concatenate(
        [
            jnp.concatenate([key_states, value_states], axis=1),
            routing_rows(expert_ids, route_weights, 2 * kv_width),
        ],
        axis=0,
    )
    from_behind, from_ahead = two_way(own_block, n_ctx)
    arrived = [own_block] + from_behind + from_ahead
    hidden_half, own_squares, routing = attend(
        ctx_rank, query_states, residual, arrived, kv_width
    )
    feat_half = hidden_half.shape[1]

    first = core == 0
    other_half, other_squares = swap(hidden_half), swap(own_squares)
    squares = own_squares[:, :1] + other_squares[:, :1]
    inv_rms = lax.rsqrt(squares / D + 1e-05)
    whole = jnp.concatenate(
        [jnp.where(first, hidden_half, other_half), jnp.where(first, other_half, hidden_half)],
        axis=1,
    )
    rows = (whole.astype(jnp.float32) * inv_rms * norm_gain[None, :]).astype(jnp.bfloat16)
    both = shift_pairs(n_ctx)
    per_chunk = tok_count // OUT_CHUNKS
    travelling = [rows[c * per_chunk : (c + 1) * per_chunk] for c in range(OUT_CHUNKS)]
    blocks = []
    for k in range(1, half_ring + 1):
        travelling = [move(x, both) for x in travelling]
        blocks.append(travelling)
        if k < half_ring:
            travelling = list(travelling)
            for c in range(1, OUT_CHUNKS):
                travelling[c], blocks[-1][c - 1] = lax.optimization_barrier(
                    (travelling[c], blocks[-1][c - 1])
                )
            if k > 1:
                travelling[0], blocks[-2][-1] = lax.optimization_barrier(
                    (travelling[0], blocks[-2][-1])
                )
    last = [
        jnp.where(first, x, rows[c * per_chunk : (c + 1) * per_chunk])
        for c, x in enumerate(blocks[-1])
    ]
    blocks[-1] = last

    routing = routing[:, :, :tok_count]
    behind = routing[1 : half_ring + 1]
    ahead = jnp.concatenate([routing[half_ring + 1 :], routing[:1]], axis=0)
    mine_marks, _ = slots_of(jnp.where(first, behind, ahead), expert, capacity)
    peer_marks, peer_weight = slots_of(jnp.where(first, ahead, behind), expert, capacity)

    per = half_ring // GROUPS
    totals = []
    for g in range(GROUPS):
        lo = g * per
        arrived_rows = jnp.stack(
            [jnp.concatenate(blocks[k], axis=0) for k in range(lo, lo + per)]
        )
        packed = jnp.einsum(
            "bst,btd->bsd",
            mine_marks[lo : lo + per],
            arrived_rows,
            preferred_element_type=jnp.float32,
        ).astype(jnp.bfloat16)
        packed = packed.reshape(per * capacity, D)
        from_peer = swap(packed)
        sent_back = swap(expert_share(packed, w_gate, w_down).astype(jnp.bfloat16))
        share = lax.optimization_barrier(expert_share(from_peer, w_gate, w_down))
        total = share + sent_back.astype(jnp.float32)
        total = total * peer_weight[lo : lo + per].reshape(-1, 1)
        totals.append(total.astype(jnp.bfloat16).reshape(per, capacity, D))

    total = jnp.concatenate(totals, axis=0)
    width = D // BACK_CHUNKS

    def in_token_form(lo, hi):
        return jnp.einsum(
            "kst,ksd->ktd", peer_marks[lo:hi], total[lo:hi], preferred_element_type=jnp.float32
        ).astype(jnp.bfloat16)

    farthest = in_token_form(half_ring - 1, half_ring)[0]
    addends = in_token_form(0, half_ring - 1)
    running = [farthest[:, c * width : (c + 1) * width] for c in range(BACK_CHUNKS)]
    for k in range(half_ring, 0, -1):
        pairs = both if k < half_ring else shift_pairs(n_ctx, (1,))
        running = [move(x, pairs) for x in running]
        if k > 1:
            running = [add_rows(x, addends, k - 2, c * width) for c, x in enumerate(running)]
    own_part = [farthest]
    gathered = jnp.concatenate(running, axis=1).astype(jnp.float32)
    gathered = gathered + jnp.where(first, jnp.concatenate(own_part, axis=0), 0).astype(jnp.float32)
    low, high = gathered[:, :feat_half], gathered[:, feat_half:]
    kept = jnp.where(first, low, high)
    given = jnp.where(first, high, low).astype(jnp.bfloat16)
    branch = kept + swap(given).astype(jnp.float32)
    return (hidden_half.astype(jnp.float32) + branch).astype(jnp.bfloat16)


def solution(mesh):
    in_specs = (
        P(("groups", "ctx"), "exp"),
        P(("groups", "ctx"), "exp"),
        P(("groups", "ctx"), "exp"),
        P(("groups", "ctx"), "exp"),
        P(),
        P(("groups", "ctx"), None),
        P(("groups", "ctx"), None),
        P(None, ("ctx", "exp")),
        P(("ctx", "exp"), None),
    )
    out_specs = P(("groups", "ctx"), "exp")
    return jax.shard_map(body, mesh=mesh, in_specs=in_specs, out_specs=out_specs, check_vma=False)
```
